32 devices in a mesh: fsdp: 2 (over x), ctx: 4 (over y, core), tp: 4 (over z).
Axes of the slice: x: 2, y: 2, z: 4, core: 2. Of those that a mesh axis runs over, the one named last changes fastest.
Arguments:
- layer_input: bfloat16 [2, 4096, 768], P('fsdp', 'ctx'), may hold values from -6 to 6
- segments: int32 [2, 4096], P('fsdp', 'ctx'), may hold values from 0 to 7, never falling along the last dimension, each value on 1 to 2048 neighbouring positions
- cotangent: bfloat16 [2, 4096, 128], P('fsdp', 'ctx'), may hold values from -64 to 64
- w_qkv: bfloat16 [3, 768, 768], P(None, 'fsdp', 'tp'), may hold values from -0.21875 to 0.21875
- b_attn: bfloat16 [2, 12, 64], P(None, 'tp', 'fsdp'), may hold values from -0.3125 to 0.3125
- w_out: bfloat16 [768, 768], P('tp', 'fsdp'), may hold values from -3 to 3
- b_out: bfloat16 [768], P('fsdp'), may hold values from -0.625 to 0.625
- ln1_gain: bfloat16 [768], P('fsdp'), may hold values from 0.5 to 1.5
- ln1_bias: bfloat16 [768], P('fsdp'), may hold values from -0.625 to 0.625
- w_in: bfloat16 [768, 3072], P('fsdp', 'tp'), may hold values from -0.21875 to 0.21875
- b_in: bfloat16 [48, 64], P('tp', 'fsdp'), may hold values from -0.625 to 0.625
- w_down: bfloat16 [3072, 768], P('tp', 'fsdp'), may hold values from -0.109375 to 0.109375
- b_down: bfloat16 [768], P('fsdp'), may hold values from -0.625 to 0.625
- ln2_gain: bfloat16 [768], P('fsdp'), may hold values from 0.5 to 1.5
- ln2_bias: bfloat16 [768], P('fsdp'), may hold values from -0.625 to 0.625
- w_proj: bfloat16 [768, 128], P('fsdp'), may hold values from -0.21875 to 0.21875
Outputs:
- embeddings: float32 [2, 4096, 128], P('fsdp', ('ctx', 'tp'))
- input_grad: float32 [2, 4096, 768], P('fsdp', ('ctx', 'tp'))
- grad_w_qkv: float32 [3, 768, 768], P(None, 'fsdp', 'tp')
- grad_b_attn: float32 [2, 12, 64], P(None, 'tp', 'fsdp')
- grad_w_out: float32 [768, 768], P('tp', 'fsdp')
- grad_b_out: float32 [768], P('fsdp')
- grad_ln1_gain: float32 [768], P('fsdp')
- grad_ln1_bias: float32 [768], P('fsdp')
- grad_w_in: float32 [768, 3072], P('fsdp', 'tp')
- grad_b_in: float32 [48, 64], P('tp', 'fsdp')
- grad_w_down: float32 [3072, 768], P('tp', 'fsdp')
- grad_b_down: float32 [768], P('fsdp')
- grad_ln2_gain: float32 [768], P('fsdp')
- grad_ln2_bias: float32 [768], P('fsdp')
- grad_w_proj: float32 [768, 128], P('fsdp')
The draws below stay inside these ranges and needn't reach their ends.
Inputs may be any that keep to these rules, and one draw needn't show every extreme that they name: `segments`: segment numbers never fall along a sequence; one document holds at most 2048 tokens.
All inputs are finite; a program needn't handle non-finite values.
Results may differ from the reference program's by a relative error of at most 0.023.
Values may be sent and summed in bfloat16 or wider, within the bound.
A program may use at most 192 MiB of HBM per device.

```python
import math
import jax
import jax.numpy as jnp
import numpy as np
from jax import lax

D = 768
H = 12
HD = 64
FF = 3072
E = 128
SEQ = 4096
DOCS = 8
MOST = 2048
SEQS = 2


def block_scale(rng, shape, pieces, smallest, top_value):
    gain, own = 1.0, jax.random.fold_in(rng, 6)
    for dim, shards_of in pieces:
        steps = jnp.exp(jax.random.uniform(jax.random.fold_in(own, dim), (shards_of,), jnp.float32, smallest / len(pieces), top_value / len(pieces)))
        gain = gain * jnp.repeat(steps, shape[dim] // shards_of).reshape([-1 if axis == dim else 1 for axis in range(len(shape))])
    return gain


def length_profile(amount, total, bound, lean):
    weights = [(1 << 20) // math.isqrt(grade ** lean) + 1 for grade in range(2, amount + 1)]
    rest, holding = total - bound - (amount - 1), [1] * (amount - 1)
    while rest > 0:
        movable = [i for i in range(amount - 1) if holding[i] < bound]
        pool, left = sum([weights[i] for i in movable]), rest
        for i in movable:
            more = min(bound - holding[i], max(1, left * weights[i] // pool), rest)
            holding[i] = holding[i] + more
            rest = rest - more
    return np.array([bound] + holding)


def uneven(key, number_of, total, reach, skew):
    if number_of == 2:
        one = jax.random.randint(key, (), max(1, total - reach), min(reach, total - 1) + 1)
        return jnp.stack([one, total - one])
    sizes = jnp.asarray(length_profile(number_of, total, reach, skew), jnp.int32)
    couples = (number_of - 1) // 2
    source_of, taker = sizes[1:1 + 2 * couples:2], sizes[2:2 + 2 * couples:2]
    margin = jnp.minimum(source_of - 1, reach - taker)
    shifted = jax.random.randint(jax.random.fold_in(key, 1), (couples,), 0, 1 << 20) % (margin + 1)
    sizes = sizes.at[1:1 + 2 * couples:2].set(source_of - shifted).at[2:2 + 2 * couples:2].set(taker + shifted)
    return sizes[jax.random.permutation(jax.random.fold_in(key, 2), number_of)]


def noise(key, extent, deviation, reach, split=(), kind=jnp.bfloat16):
    array = jax.random.normal(key, extent, jnp.float32) * deviation
    if len(split) > 0:
        array = block_scale(key, extent, split, -0.22, 0.18) * array
    return jnp.clip(array, min=-reach, max=reach).astype(kind)


def setup_inputs(seed: int = 0) -> dict:
    splits = jax.random.split(jax.random.key(seed), 17)
    return {
        "layer_input": noise(splits[0], (SEQS, SEQ, D), 1.0, 6.0, ((0, 2), (1, 4))),
        "segments": jax.vmap(lambda own: jnp.searchsorted(jnp.cumsum(uneven(own, DOCS, SEQ, MOST, 1)), jnp.arange(SEQ), side="right"))(jax.random.split(splits[1], SEQS)).reshape((SEQS, SEQ)).astype(jnp.int32),
        "cotangent": noise(splits[2], (SEQS, SEQ, E), 10.0, 64.0, ((0, 2), (1, 4))),
        "w_qkv": noise(splits[3], (3, D, D), D ** -0.5, 0.21875, ((1, 2), (2, 4))),
        "b_attn": noise(splits[4], (2, H, HD), 0.05, 0.3125, ((1, 4), (2, 2))),
        "w_out": noise(splits[5], (D, D), 4 ** -0.5, 3.0, ((0, 4), (1, 2))),
        "b_out": noise(splits[6], (D,), 0.1, 0.625, ((0, 2),)),
        "ln1_gain": jnp.clip(1.0 + 0.1 * jax.random.normal(splits[7], (D,), jnp.float32), 0.5, 1.5).astype(jnp.bfloat16),
        "ln1_bias": noise(splits[8], (D,), 0.1, 0.625, ((0, 2),)),
        "w_in": noise(splits[9], (D, FF), D ** -0.5, 0.21875, ((0, 2), (1, 4))),
        "b_in": noise(splits[10], (FF // HD, HD), 0.1, 0.625, ((0, 4), (1, 2))),
        "w_down": noise(splits[11], (FF, D), FF ** -0.5, 0.109375, ((0, 4), (1, 2))),
        "b_down": noise(splits[12], (D,), 0.1, 0.625, ((0, 2),)),
        "ln2_gain": jnp.clip(1.0 + 0.1 * jax.random.normal(splits[13], (D,), jnp.float32), 0.5, 1.5).astype(jnp.bfloat16),
        "ln2_bias": noise(splits[14], (D,), 0.1, 0.625, ((0, 2),)),
        "w_proj": noise(splits[15], (D, E), D ** -0.5, 0.21875, ((0, 2),)),
    }


LN_EPS = 1e-05
NORM_EPS = 1e-06
MASKED = -1e+30
HIGHEST_PREC = lax.Precision.HIGHEST

@jax.custom_vjp
def low(v):
    return lax.optimization_barrier(v.astype(jnp.bfloat16)).astype(jnp.float32)

@jax.custom_vjp
def low_back(v):
    return v

def low_keep(v):
    return (low(v), None)

def low_pass(kept, grad):
    return (grad,)

def back_keep(v):
    return (v, None)

def back_low(kept, grad):
    return (low(grad),)
low.defvjp(low_keep, low_pass)
low_back.defvjp(back_keep, back_low)

def round_both(value):
    return low(low_back(value))

def matmul_hi(former, latter):
    return jnp.dot(former, latter, precision=HIGHEST_PREC)

def layer_norm(resid, gain_vec, bias_vec):
    row_mean = lax.optimization_barrier(jnp.mean(resid, -1, keepdims=True))
    centred = resid - row_mean
    row_var = lax.optimization_barrier(jnp.mean(centred * centred, -1, keepdims=True))
    return centred * lax.rsqrt(row_var + LN_EPS) * gain_vec + bias_vec

def forward(params, tokens, seg_row):
    w_qkv, b_attn, w_out, b_out, ln1_gain, ln1_bias, w_in, b_in, w_down, b_down, ln2_gain, ln2_bias, w_proj = params
    query = round_both(matmul_hi(tokens, w_qkv[0]) + b_attn[0].reshape(D))
    keys = round_both(matmul_hi(tokens, w_qkv[1]))
    values = round_both(matmul_hi(tokens, w_qkv[2]) + b_attn[1].reshape(D))
    block_rows = min(512, SEQ)
    query_blocks = query.reshape(SEQ // block_rows, block_rows, H, HD)
    seg_blocks = seg_row.reshape(SEQ // block_rows, block_rows)
    key_heads = keys.reshape(SEQ, H, HD)
    value_heads = values.reshape(SEQ, H, HD)

    def attend(pair):
        query_block, seg_block = pair
        scores = jnp.einsum('qhd,khd->hqk', query_block, key_heads, precision=HIGHEST_PREC) * HD ** (-0.5)
        scores = low_back(scores)
        same_doc = seg_block[:, None] == seg_row[None, :]
        scores = jnp.where(same_doc[None], scores, MASKED)
        prob_rows = jax.nn.softmax(scores, axis=-1)
        return jnp.einsum('hqk,khd->qhd', low(prob_rows), value_heads, precision=HIGHEST_PREC)
    attended = round_both(lax.map(jax.checkpoint(attend), (query_blocks, seg_blocks)).reshape(SEQ, D))
    branch_one = low_back(matmul_hi(attended, w_out) + b_out)
    first = layer_norm(tokens + branch_one, ln1_gain, ln1_bias)
    hidden = low_back(matmul_hi(low(first), w_in) + b_in.reshape(FF))
    activated = low(jax.nn.gelu(hidden, approximate=False))
    branch_two = low_back(matmul_hi(activated, w_down) + b_down)
    second = layer_norm(first + branch_two, ln2_gain, ln2_bias)
    projected = low_back(matmul_hi(low(second), w_proj))
    return projected * lax.rsqrt(lax.optimization_barrier(jnp.sum(projected * projected, -1, keepdims=True)) + NORM_EPS)

def reference(layer_input, segments, cotangent, w_qkv, b_attn, w_out, b_out, ln1_gain, ln1_bias, w_in, b_in, w_down, b_down, ln2_gain, ln2_bias, w_proj):
    params = (w_qkv.astype(jnp.float32), b_attn.astype(jnp.float32), w_out.astype(jnp.float32), b_out.astype(jnp.float32), ln1_gain.astype(jnp.float32), ln1_bias.astype(jnp.float32), w_in.astype(jnp.float32), b_in.astype(jnp.float32), w_down.astype(jnp.float32), b_down.astype(jnp.float32), ln2_gain.astype(jnp.float32), ln2_bias.astype(jnp.float32), w_proj.astype(jnp.float32))

    def per_sequence(grad_total, sequence_item):
        token_row, seg_row, cotan_row = sequence_item
        embedded, pullback = jax.vjp(lambda weights_all, inputs_all: forward(weights_all, inputs_all, seg_row), params, token_row.astype(jnp.float32))
        grad_params, grad_input = pullback(cotan_row.astype(jnp.float32))
        return (jax.tree.map(jnp.add, grad_total, grad_params), (embedded, grad_input))
    zero_grads = jax.tree.map(jnp.zeros_like, params)
    totals, (embeddings, input_grad) = lax.scan(per_sequence, zero_grads, (layer_input, segments, cotangent))
    return (embeddings, input_grad, totals[0], totals[1], totals[2], totals[3], totals[4], totals[5], totals[6], totals[7], totals[8], totals[9], totals[10], totals[11], totals[12])
```

```python
import functools
import jax
import jax.numpy as jnp
from jax import lax
from jax.experimental import pallas as pl
from jax.experimental.pallas import tpu as pltpu
from jax.sharding import PartitionSpec as P

HD = 64
LN_EPS = 1e-05
NORM_EPS = 1e-06
SQRT_HALF = 0.7071067811865476
PDF_SCALE = 0.3989422804014327
SCORE_LOG2 = 0.125 * 1.4426950408889634
MASKED = -1e30
QB = 512
KB = 512
SEGS = 8


def dot_ab(a, b):
    return lax.dot_general(a, b, (((1,), (0,)), ((), ())), preferred_element_type=jnp.float32)


def dot_abt(a, b):
    return lax.dot_general(a, b, (((1,), (1,)), ((), ())), preferred_element_type=jnp.float32)


def eye(rows, cols, shift):
    r = lax.broadcasted_iota(jnp.int32, (rows, cols), 0)
    c = lax.broadcasted_iota(jnp.int32, (rows, cols), 1)
    return jnp.where(r + shift == c, 1.0, 0.0).astype(jnp.bfloat16)


def spread_keys(kv_ref, segk_ref, block, kaug_ref, base, width):
    ident = eye(KB, KB, 0)
    for sub in range(kv_ref.shape[0] // KB):
        rows = pl.ds(sub * KB, KB)
        seg_row = segk_ref[block : block + 1, sub * KB : (sub + 1) * KB]
        tag = lax.broadcasted_iota(jnp.int32, (128, KB), 0) - (width - 128)
        hot = jnp.where(tag == seg_row, 1.0, 0.0).astype(jnp.bfloat16)
        hot_cols = dot_abt(ident, hot).astype(jnp.bfloat16)
        lane = lax.broadcasted_iota(jnp.int32, (KB, 128), 1)
        own = kv_ref[rows, 128:256]
        kaug_ref[pl.ds(base + sub * KB, KB), 0:128] = kv_ref[rows, 0:128]
        kaug_ref[pl.ds(base + sub * KB, KB), 128:256] = jnp.where(
            lane < width - 128, own, hot_cols
        )


def masked_query(q_cols, seg_row, head):
    width = q_cols.shape[0]
    row = lax.broadcasted_iota(jnp.int32, (width, QB), 0)
    inside = (row >= head * HD) & (row < (head + 1) * HD)
    tag = lax.broadcasted_iota(jnp.int32, (256 - width, QB), 0)
    bias = jnp.where((tag < SEGS) & (tag != seg_row), MASKED, 0.0).astype(jnp.bfloat16)
    return jnp.concatenate([jnp.where(inside, q_cols, jnp.zeros_like(q_cols)), bias], 0)


def overlaps(segs_q, q_first, segs_k, block, k_first):
    q_low, q_high = segs_q[0, q_first], segs_q[0, q_first + QB - 1]
    return (segs_k[block, k_first] <= q_high) & (segs_k[block, k_first + KB - 1] >= q_low)


def forward_kernel(nb, first, last, *refs):
    segs_q, segs_k, segq_ref, segk_ref, q_ref = refs[:5]
    kv_refs = refs[5 : 5 + nb]
    pos = 5 + nb
    if not first:
        m_in, l_in, acc_in = refs[pos : pos + 3]
        pos += 3
    outs = refs[pos : pos + (2 if last else 3)]
    pos += 2 if last else 3
    kaug_ref, vt_ref, m_ref, l_ref, acc_ref = refs[pos:]
    width = q_ref.shape[0]
    heads = width // HD
    step = pl.program_id(0)
    rows = kv_refs[0].shape[0]
    q_first = step * QB

    @pl.when(step == 0)
    def _():
        pick = eye(width, 2 * width, width)
        for block in range(nb):
            spread_keys(kv_refs[block], segk_ref, block, kaug_ref, block * rows, width)
            for sub in range(rows // KB):
                vt_ref[:, block * rows + sub * KB : block * rows + (sub + 1) * KB] = dot_abt(
                    pick, kv_refs[block][sub * KB : (sub + 1) * KB, :]
                ).astype(jnp.bfloat16)

    if first:
        m_ref[...] = jnp.full_like(m_ref, -3e38)
        l_ref[...] = jnp.zeros_like(l_ref)
        acc_ref[...] = jnp.zeros_like(acc_ref)
    else:
        m_ref[...] = m_in[...]
        l_ref[...] = l_in[...]
        acc_ref[...] = acc_in[...]
    seg_row = segq_ref[0:1, :]
    q_heads = [masked_query(q_ref[...], seg_row, h) for h in range(heads)]
    for block in range(nb):

        def body(sub, carry, block=block):
            @pl.when(overlaps(segs_q, q_first, segs_k, block, sub * KB))
            def _():
                at = pl.multiple_of(block * rows + sub * KB, KB)
                keys = kaug_ref[pl.ds(at, KB), :]
                for h in range(heads):
                    scores = dot_ab(keys, q_heads[h]) * SCORE_LOG2
                    old = m_ref[h : h + 1, :]
                    new = jnp.maximum(old, jnp.max(scores, 0, keepdims=True))
                    probs = jnp.exp2(scores - new)
                    alpha = jnp.exp2(old - new)
                    m_ref[h : h + 1, :] = new
                    l_ref[h : h + 1, :] = l_ref[h : h + 1, :] * alpha + jnp.sum(
                        probs, 0, keepdims=True
                    )
                    acc_ref[h * HD : (h + 1) * HD, :] = acc_ref[
                        h * HD : (h + 1) * HD, :
                    ] * alpha + dot_ab(
                        vt_ref[h * HD : (h + 1) * HD, pl.ds(at, KB)], probs.astype(jnp.bfloat16)
                    )

            return carry

        lax.fori_loop(0, rows // KB, body, 0)
    if last:
        out_ref, lse_ref = outs
        lse_ref[...] = jnp.zeros_like(lse_ref)
        for h in range(heads):
            total = l_ref[h : h + 1, :]
            out_ref[h * HD : (h + 1) * HD, :] = (
                acc_ref[h * HD : (h + 1) * HD, :] / total
            ).astype(jnp.bfloat16)
            lse_ref[h : h + 1, :] = m_ref[h : h + 1, :] + jnp.log2(total)
    else:
        outs[0][...] = m_ref[...]
        outs[1][...] = l_ref[...]
        outs[2][...] = acc_ref[...]


def attend_forward(segs_q, segs_k, q_cols, kvs, carry, last):
    nb = len(kvs)
    width, count = q_cols.shape
    rows = kvs[0].shape[0]
    first = carry is None
    smem = pl.BlockSpec(memory_space=pltpu.SMEM)
    vec = lambda r: pl.BlockSpec((r, QB), lambda i: (0, i))
    whole = lambda a: pl.BlockSpec(a.shape, lambda i: (0, 0))
    args = [segs_q, segs_k, segs_q, segs_k, q_cols, *kvs]
    specs = [smem, smem, vec(1), whole(segs_k), vec(width), *[whole(k) for k in kvs]]
    if not first:
        args += list(carry)
        specs += [vec(8), vec(8), vec(width)]
    f32 = jnp.float32
    if last:
        out_shape = (
            jax.ShapeDtypeStruct((width, count), jnp.bfloat16),
            jax.ShapeDtypeStruct((8, count), f32),
        )
        out_specs = (vec(width), vec(8))
    else:
        out_shape = (
            jax.ShapeDtypeStruct((8, count), f32),
            jax.ShapeDtypeStruct((8, count), f32),
            jax.ShapeDtypeStruct((width, count), f32),
        )
        out_specs = (vec(8), vec(8), vec(width))
    return pl.pallas_call(
        functools.partial(forward_kernel, nb, first, last),
        grid=(count // QB,),
        in_specs=specs,
        out_specs=out_specs,
        out_shape=out_shape,
        scratch_shapes=[
            pltpu.VMEM((nb * rows, 256), jnp.bfloat16),
            pltpu.VMEM((width, nb * rows), jnp.bfloat16),
            pltpu.VMEM((8, QB), f32),
            pltpu.VMEM((8, QB), f32),
            pltpu.VMEM((width, QB), f32),
        ],
        compiler_params=pltpu.CompilerParams(vmem_limit_bytes=24 << 20),
        cost_estimate=pl.CostEstimate(
            flops=4 * count * rows * nb * width, bytes_accessed=nb * rows * width * 4,
            transcendentals=count * rows * nb * 3,
        ),
        name="attend_forward",
    )(*args)


def backward_kernel(nb, first, last, *refs):
    segs_q, segs_k, segq_ref, segk_ref, q_ref, d_out_ref, out_ref, lse_ref = refs[:8]
    kv_refs = refs[8 : 8 + nb]
    pos = 8 + nb
    if not first:
        dq_in = refs[pos]
        pos += 1
    dq_ref = refs[pos]
    dkv_refs = refs[pos + 1 : pos + 1 + nb]
    pos += 1 + nb
    kaug_ref, kt_ref, acc_ref, dq_acc = refs[pos:]
    width = q_ref.shape[0]
    heads = width // HD
    step = pl.program_id(0)
    rows = kv_refs[0].shape[0]
    q_first = step * QB
    bf = jnp.bfloat16

    @pl.when(step == 0)
    def _():
        pick = eye(width, 2 * width, 0)
        acc_ref[...] = jnp.zeros_like(acc_ref)
        for block in range(nb):
            spread_keys(kv_refs[block], segk_ref, block, kaug_ref, block * rows, width)
            for sub in range(rows // KB):
                kt_ref[:, block * rows + sub * KB : block * rows + (sub + 1) * KB] = dot_abt(
                    pick, kv_refs[block][sub * KB : (sub + 1) * KB, :]
                ).astype(bf)

    seg_row = segq_ref[0:1, :]
    q_cols, d_cols = q_ref[...], d_out_ref[...]
    ident = eye(QB, QB, 0)
    pad = jnp.zeros((256 - width, QB), bf)
    q_nat = dot_abt(ident, jnp.concatenate([q_cols, pad], 0)).astype(bf)
    d_nat = dot_abt(ident, jnp.concatenate([pad, d_cols], 0)).astype(bf)
    row = lax.broadcasted_iota(jnp.int32, (256, QB), 0)
    lane = lax.broadcasted_iota(jnp.int32, (QB, 256), 1)
    off = 256 - width
    d_full = jnp.concatenate([pad, d_cols], 0)
    zero = jnp.zeros((QB, 256), bf)
    q_heads, q_rows, d_heads, d_rows, deltas = [], [], [], [], []
    for h in range(heads):
        q_heads.append(masked_query(q_cols, seg_row, h))
        q_rows.append(jnp.where((lane >= h * HD) & (lane < (h + 1) * HD), q_nat, zero))
        d_heads.append(
            jnp.where((row >= off + h * HD) & (row < off + (h + 1) * HD), d_full, jnp.zeros_like(d_full))
        )
        d_rows.append(jnp.where((lane >= off + h * HD) & (lane < off + (h + 1) * HD), d_nat, zero))
        part = slice(h * HD, (h + 1) * HD)
        deltas.append(
            jnp.sum(
                d_out_ref[part, :].astype(jnp.float32) * out_ref[part, :].astype(jnp.float32),
                0,
                keepdims=True,
            )
        )
    if first:
        dq_acc[...] = jnp.zeros_like(dq_acc)
    else:
        dq_acc[...] = dq_in[...]
    for block in range(nb):

        def body(sub, carry, block=block):
            @pl.when(overlaps(segs_q, q_first, segs_k, block, sub * KB))
            def _():
                at = pl.multiple_of(block * rows + sub * KB, KB)
                here = pl.ds(pl.multiple_of(sub * KB, KB), KB)
                keys = kaug_ref[pl.ds(at, KB), :]
                vals = kv_refs[block][here, 2 * width - 256 : 2 * width]
                for h in range(heads):
                    scores = dot_ab(keys, q_heads[h]) * SCORE_LOG2
                    probs = jnp.exp2(scores - lse_ref[h : h + 1, :])
                    d_probs = dot_ab(vals, d_heads[h])
                    d_scores = (probs * (d_probs - deltas[h])).astype(bf)
                    acc_ref[pl.ds(at, KB), 0:256] += dot_ab(d_scores, q_rows[h])
                    acc_ref[pl.ds(at, KB), 2 * width - 256 : 2 * width] += dot_ab(
                        probs.astype(bf), d_rows[h]
                    )
                    part = slice(h * HD, (h + 1) * HD)
                    dq_acc[part, :] += dot_ab(kt_ref[part, pl.ds(at, KB)], d_scores)

            return carry

        lax.fori_loop(0, rows // KB, body, 0)
    if last:
        dq_ref[...] = (dq_acc[...] * 0.125).astype(bf)
    else:
        dq_ref[...] = dq_acc[...]

    @pl.when(step == pl.num_programs(0) - 1)
    def _():
        key_lane = lax.broadcasted_iota(jnp.int32, (KB, 2 * width), 1)
        scale = jnp.where(key_lane < width, 0.125, 1.0)
        for block in range(nb):
            for sub in range(rows // KB):
                dkv_refs[block][sub * KB : (sub + 1) * KB, :] = (
                    acc_ref[block * rows + sub * KB : block * rows + (sub + 1) * KB, :] * scale
                ).astype(dkv_refs[block].dtype)


def attend_backward(segs_q, segs_k, q_cols, d_out, out, lse, kvs, dq, last, types):
    nb = len(kvs)
    width, count = q_cols.shape
    rows = kvs[0].shape[0]
    first = dq is None
    smem = pl.BlockSpec(memory_space=pltpu.SMEM)
    vec = lambda r: pl.BlockSpec((r, QB), lambda i: (0, i))
    whole = lambda a: pl.BlockSpec(a.shape, lambda i: (0, 0))
    args = [segs_q, segs_k, segs_q, segs_k, q_cols, d_out, out, lse, *kvs]
    specs = [smem, smem, vec(1), whole(segs_k), vec(width), vec(width), vec(width), vec(8)]
    specs += [whole(k) for k in kvs]
    if not first:
        args.append(dq)
        specs.append(vec(width))
    f32 = jnp.float32
    out_shape = [jax.ShapeDtypeStruct((width, count), jnp.bfloat16 if last else f32)]
    out_shape += [jax.ShapeDtypeStruct((rows, 2 * width), t) for t in types]
    out_specs = [vec(width)] + [whole(k) for k in kvs]
    return pl.pallas_call(
        functools.partial(backward_kernel, nb, first, last),
        grid=(count // QB,),
        in_specs=specs,
        out_specs=out_specs,
        out_shape=out_shape,
        scratch_shapes=[
            pltpu.VMEM((nb * rows, 256), jnp.bfloat16),
            pltpu.VMEM((width, nb * rows), jnp.bfloat16),
            pltpu.VMEM((nb * rows, 2 * width), f32),
            pltpu.VMEM((width, QB), f32),
        ],
        compiler_params=pltpu.CompilerParams(vmem_limit_bytes=40 << 20),
        cost_estimate=pl.CostEstimate(
            flops=10 * count * rows * nb * width, bytes_accessed=nb * rows * width * 8,
            transcendentals=count * rows * nb * 3,
        ),
        name="attend_backward",
    )(*args)


def exchange(value, axis, flip):
    size = lax.axis_size(axis)
    return lax.ppermute(value, axis, [(i, i ^ flip) for i in range(size)])


def rotate(value, axis, amount):
    size = lax.axis_size(axis)
    return lax.ppermute(value, axis, [(i, (i + amount) % size) for i in range(size)])


def in_order(index, own, other, dim):
    first = index == 0
    return jnp.concatenate([jnp.where(first, own, other), jnp.where(first, other, own)], dim)


def part(array, index, count, dim):
    size = array.shape[dim] // count
    return lax.dynamic_slice_in_dim(array, index * size, size, dim)


def pad_to(array, rows, cols):
    return jnp.pad(array, ((0, rows - array.shape[0]), (0, cols - array.shape[1])))


def low(value):
    return value.astype(jnp.bfloat16)


def wide(value):
    return value.astype(jnp.float32)


def sum_pair(value, axis, flip):
    rounded = low(value)
    return wide(rounded) + wide(exchange(rounded, axis, flip))


def gather_attention(w_qkv, b_attn, w_proj, vectors, core):
    width = w_qkv.shape[2]
    main = jnp.concatenate([w_qkv[0], w_qkv[1], w_qkv[2], w_proj], 1)
    cols = main.shape[1]
    bias = b_attn.reshape(2 * b_attn.shape[1], b_attn.shape[2])
    if lax.axis_size("fsdp") != 2:
        weights = lax.all_gather(main, "fsdp", axis=0, tiled=True)
        vecs = lax.all_gather(vectors, "fsdp", axis=1, tiled=True)
        biases = lax.all_gather(bias, "fsdp", axis=1, tiled=True)
        return weights, vecs, biases.reshape(2, width)
    side = lax.axis_index("fsdp")
    half = main.shape[0] // 2
    wide_cols = -(-cols // 128) * 128
    small = jnp.concatenate(
        [
            pad_to(vectors, 8, wide_cols - 128),
            pad_to(bias, 8, wide_cols - 128),
        ],
        0,
    )
    packed = jnp.concatenate(
        [pad_to(part(main, core, 2, 0), half, wide_cols), pad_to(small, 16, wide_cols)], 0
    )
    got = exchange(packed, "fsdp", 1)
    got_half = got[:half]
    partner_half = exchange(got_half, "ctx", 1)
    other = in_order(core, got_half, partner_half, 0)[:, :cols]
    weights = in_order(side, main, other, 0)
    length = vectors.shape[1]
    vecs = in_order(side, vectors, got[half : half + 6, :length], 1)
    biases = in_order(
        side, bias, got[half + 8 : half + 8 + bias.shape[0], : bias.shape[1]], 1
    )
    return weights, vecs, biases.reshape(2, width)


def gather_ffn(w_in, w_down, w_out, b_in, core):
    steps = lax.axis_size("tp")
    half = w_down.shape[0] // 2
    out_half = w_out.shape[0] // 2
    into = part(w_in, core, 2, 1)
    down = part(w_down, core, 2, 0)
    outer = part(w_out, core, 2, 0)
    rows = b_in.shape[0]
    if lax.axis_size("fsdp") != 2:
        pieces = [
            (
                lax.all_gather(into, "fsdp", axis=0, tiled=True),
                lax.all_gather(down, "fsdp", axis=1, tiled=True),
                lax.all_gather(outer, "fsdp", axis=1, tiled=True),
                lax.all_gather(b_in, "fsdp", axis=1, tiled=True),
            )
        ]
        for _ in range(steps - 1):
            pieces.append(tuple(rotate(a, "tp", 1) for a in pieces[-1]))
    else:
        side = lax.axis_index("fsdp")
        depth = w_in.shape[0]
        packed = [
            jnp.concatenate([into, down, outer, pad_to(b_in, 16, depth)], 0)
        ]
        for _ in range(steps - 1):
            packed.append(rotate(packed[-1], "tp", 1))
        pieces = []
        for own in packed:
            other = exchange(own, "fsdp", 1)
            a, b = depth + half, depth + half + out_half
            pieces.append(
                (
                    in_order(side, own[:depth], other[:depth], 0),
                    in_order(side, own[depth:a], other[depth:a], 1),
                    in_order(side, own[a:b], other[a:b], 1),
                    in_order(
                        side,
                        own[b : b + rows, : b_in.shape[1]],
                        other[b : b + rows, : b_in.shape[1]],
                        1,
                    ),
                )
            )
    outers = jnp.stack([p[2] for p in pieces])
    partner = exchange(outers, "ctx", 1)
    full_out = in_order(core, outers, partner, 1).reshape(steps * 2 * out_half, -1)
    w_into = jnp.concatenate([p[0] for p in pieces], 1)
    w_downs = jnp.concatenate([p[1] for p in pieces], 0)
    bias = jnp.concatenate([part(p[3], core, 2, 0).reshape(-1) for p in pieces])
    return w_into, w_downs, full_out, wide(bias)


def reduce_ffn(g_into, g_down, g_bias, g_out, g_proj, g_vecs, core):
    steps = lax.axis_size("tp")
    model = g_into.shape[0]
    half = g_down.shape[0] // steps
    out_rows = g_out.shape[0] // steps
    outs = low(g_out).reshape(steps, 2, out_rows // 2, model)
    take = lambda a, i, d: lax.dynamic_index_in_dim(a, i, d, keepdims=False)
    out_mine = take(outs, core, 1).reshape(-1, model)
    out_sent = take(outs, 1 - core, 1).reshape(-1, model)
    embed = g_proj.shape[1]
    proj_cols = jnp.concatenate([low(g_proj).T, pad_to(low(g_vecs), 16, model)], 0)
    got = exchange(jnp.concatenate([out_sent, proj_cols], 0), "ctx", 1)
    count = out_sent.shape[0]
    out_sum = low(wide(out_mine) + wide(got[:count])).reshape(steps, out_rows // 2, model)
    proj_sum = wide(proj_cols) + wide(got[count:])
    proj_half = low(part(proj_sum[:embed], core, 2, 0))
    tail = jnp.concatenate([proj_half, low(proj_sum[embed:])], 0)
    into, down = low(g_into), low(g_down)
    rows = half // HD
    if lax.axis_size("fsdp") != 2:
        scatter = lambda a, d: lax.psum_scatter(low(a), "fsdp", scatter_dimension=d, tiled=True)
        depth = model // lax.axis_size("fsdp")
        packs = []
        biases = []
        for s in range(steps):
            packs.append(
                jnp.concatenate(
                    [
                        scatter(into[:, s * half : (s + 1) * half], 0).T,
                        scatter(down[s * half : (s + 1) * half], 1),
                        scatter(out_sum[s], 1),
                        scatter(tail, 1),
                    ],
                    0,
                )
            )
            biases.append(
                scatter(low(g_bias[s * half : (s + 1) * half]).reshape(rows, HD), 1)
            )
        total, bias = packs[-1], biases[-1]
        for s in range(steps - 2, -1, -1):
            total = low(wide(rotate(total, "tp", -1)) + wide(packs[s]))
            bias = low(wide(rotate(bias, "tp", -1)) + wide(biases[s]))
        span = half
    else:
        side = lax.axis_index("fsdp")
        depth = model // 2
        span = depth

        def pack(index, s):
            cut = slice(s * half, (s + 1) * half)
            bias_rows = part(low(g_bias[cut]).reshape(rows, HD), index, 2, 1)
            return jnp.concatenate(
                [
                    part(into[:, cut], index, 2, 0),
                    part(down[cut], index, 2, 1),
                    part(out_sum[s], index, 2, 1),
                    part(tail, index, 2, 1),
                    pad_to(bias_rows, 16, depth),
                ],
                0,
            )

        total = None
        for s in range(steps - 1, -1, -1):
            got = exchange(pack(1 - side, s), "fsdp", 1)
            here = wide(pack(side, s)) + wide(got)
            if total is not None:
                here = here + wide(rotate(total, "tp", -1))
            total = low(here)
    total = low(sum_pair(total, "ctx", 2))
    if lax.axis_size("fsdp") == 2:
        other = exchange(total, "ctx", 1)
    else:
        bias = low(sum_pair(bias, "ctx", 2))
        other = exchange(total, "ctx", 1)
        bias = in_order(core, bias, exchange(bias, "ctx", 1), 0)
    at = [0, span, span + half, span + half + out_rows // 2]
    at += [at[-1] + embed // 2, at[-1] + embed // 2 + 16]
    both = lambda i, d: in_order(
        core, total[at[i] : at[i + 1]], other[at[i] : at[i + 1]], d
    )
    if lax.axis_size("fsdp") == 2:
        grad_in = both(0, 1)
        grad_bias = in_order(
            core, total[at[5] : at[5] + rows, : HD // 2], other[at[5] : at[5] + rows, : HD // 2], 0
        )
    else:
        grad_in = both(0, 0).T
        grad_bias = bias
    return (
        wide(grad_in),
        wide(both(1, 0)),
        wide(grad_bias),
        wide(both(2, 0)),
        wide(both(3, 0)).T,
        wide(total[at[4] : at[4] + 6]),
    )


def reduce_attention(g_main, g_bias, core):
    model, cols = g_main.shape
    bias = pad_to(g_bias.reshape(1, -1), 16, cols)
    if lax.axis_size("fsdp") != 2:
        own = lax.psum_scatter(low(g_main), "fsdp", scatter_dimension=0, tiled=True)
        shared = lax.psum(low(bias), "fsdp")
        both = jnp.concatenate([own, shared], 0)
        both = low(sum_pair(both, "ctx", 1))
        both = sum_pair(both, "ctx", 2)
        count = own.shape[0]
        return wide(low(both[:count])), both[count]
    side = lax.axis_index("fsdp")
    quarter = model // 4
    quads = low(g_main).reshape(2, 2, quarter, cols)
    take = lambda a, i, d: lax.dynamic_index_in_dim(a, i, d, keepdims=False)
    mine, sent = take(quads, core, 1), take(quads, 1 - core, 1)
    got = exchange(
        jnp.concatenate([sent.reshape(2 * quarter, cols), low(bias)], 0), "ctx", 1
    )
    halves = wide(mine) + wide(got[: 2 * quarter]).reshape(2, quarter, cols)
    bias = low(wide(low(bias)) + wide(got[2 * quarter :]))
    sent = jnp.concatenate([low(take(halves, 1 - side, 0)), bias], 0)
    got = exchange(sent, "fsdp", 1)
    own = take(halves, side, 0) + wide(got[:quarter])
    bias = low(wide(bias) + wide(got[quarter:]))
    both = low(sum_pair(jnp.concatenate([low(own), bias], 0), "ctx", 2))
    other = exchange(both[:quarter], "ctx", 1)
    return wide(in_order(core, both[:quarter], other, 0)), wide(both[quarter])


def normalize(resid, gain_vec, bias_vec):
    row_mean = jnp.mean(resid, -1, keepdims=True)
    centred = resid - row_mean
    inv_dev = lax.rsqrt(jnp.mean(centred * centred, -1, keepdims=True) + LN_EPS)
    normed = centred * inv_dev
    return (normed * gain_vec + bias_vec, normed, inv_dev)


def normalize_back(upstream, normed, inv_dev, gain_vec):
    scaled = upstream * gain_vec
    back_grad = inv_dev * (
        scaled
        - jnp.mean(scaled, -1, keepdims=True)
        - normed * jnp.mean(scaled * normed, -1, keepdims=True)
    )
    return (back_grad, jnp.sum(upstream * normed, 0), jnp.sum(upstream, 0))


def dot_atb(a, b):
    return lax.dot_general(a, b, (((0,), (0,)), ((), ())), preferred_element_type=jnp.float32)


def dot_atbt(a, b):
    return lax.dot_general(a, b, (((0,), (1,)), ((), ())), preferred_element_type=jnp.float32)


def shards(
    layer_input,
    segments,
    cotangent,
    w_qkv,
    b_attn,
    w_out,
    b_out,
    ln1_gain,
    ln1_bias,
    w_in,
    b_in,
    w_down,
    b_down,
    ln2_gain,
    ln2_bias,
    w_proj,
):
    _, count, model = layer_input.shape
    width = w_qkv.shape[2]
    steps = lax.axis_size("tp")
    share = count // steps
    t_index = lax.axis_index("tp")
    core = lax.axis_index("ctx") % 2
    tokens = layer_input.reshape(count, model)
    own_tokens = part(tokens, t_index, steps, 0)
    upstream = wide(part(cotangent.reshape(count, -1), t_index, steps, 0))

    seg_own = segments.reshape(1, count)
    vectors = jnp.stack([b_out, ln1_gain, ln1_bias, b_down, ln2_gain, ln2_bias])
    weights, vecs, biases = gather_attention(w_qkv, b_attn, w_proj, vectors, core)
    seg_y = exchange(seg_own, "ctx", 2)
    seg_pair = exchange(jnp.concatenate([seg_own, seg_y], 0), "ctx", 1)
    seg_near = jnp.concatenate([seg_own, seg_pair[0:1]], 0)
    seg_far = jnp.concatenate([seg_y, seg_pair[1:2]], 0)

    w_q, w_kv = weights[:, :width], weights[:, width : 3 * width]
    wproj_full = weights[:, 3 * width :]
    bout_vec, gain_one, shift_one, bdown_vec, gain_two, shift_two = [wide(vecs[i]) for i in range(6)]
    kv_bias = jnp.concatenate([jnp.zeros((width,), jnp.float32), wide(biases[1])])
    kv_own = low(dot_ab(tokens, w_kv) + kv_bias)
    kv_y = exchange(kv_own, "ctx", 2)
    kv_c = exchange(kv_own, "ctx", 1)
    q_cols = low(dot_atbt(w_q, tokens) + wide(biases[0])[:, None])
    kv_yc = exchange(kv_y, "ctx", 1)
    w_into, w_downs, wout_full, bin_vec = gather_ffn(w_in, w_down, w_out, b_in, core)

    carry = attend_forward(seg_own, seg_near, q_cols, [kv_own, kv_c], None, False)
    out_cols, lse = attend_forward(seg_own, seg_far, q_cols, [kv_y, kv_yc], carry, True)

    cut = lambda j: part(out_cols, j % steps, steps, 1)
    attended = jnp.concatenate(
        [cut(t_index)] + [rotate(cut(t_index + s), "tp", s) for s in range(1, steps)], 0
    )
    branch_one = dot_atb(attended, wout_full) + bout_vec
    first, normed_one, inv_one = normalize(wide(own_tokens) + branch_one, gain_one, shift_one)
    first_low = low(first)
    first_both = jnp.concatenate([first_low, exchange(first_low, "ctx", 1)], 0)
    hidden = dot_ab(first_both, w_into) + bin_vec
    activated = low(jax.nn.gelu(hidden, approximate=False))
    partial = dot_ab(activated, w_downs)
    branch_two = partial[:share] + wide(exchange(low(partial[share:]), "ctx", 1)) + bdown_vec
    second, normed_two, inv_two = normalize(first + branch_two, gain_two, shift_two)
    second_low = low(second)
    projected = dot_ab(second_low, wproj_full)
    proj_inv = lax.rsqrt(jnp.sum(projected * projected, -1, keepdims=True) + NORM_EPS)
    embedded = projected * proj_inv
    d_proj = low(
        proj_inv * (upstream - embedded * jnp.sum(embedded * upstream, -1, keepdims=True))
    )
    grad_wproj = dot_atb(second_low, d_proj)
    d_second = dot_abt(d_proj, wproj_full)
    d_res_two, grad_gain_two, grad_shift_two = normalize_back(
        d_second, normed_two, inv_two, gain_two
    )
    d_rows = low(d_res_two)
    grad_bdown = jnp.sum(wide(d_rows), 0)
    d_both = jnp.concatenate([d_rows, exchange(d_rows, "ctx", 1)], 0)
    d_activated = dot_abt(d_both, w_downs)
    normal_cdf = 0.5 * (1.0 + lax.erf(hidden * SQRT_HALF))
    normal_pdf = jnp.exp(-0.5 * hidden * hidden) * PDF_SCALE
    d_hidden = low(d_activated * (normal_cdf + hidden * normal_pdf))
    back = dot_abt(d_hidden, w_into)
    d_first = d_res_two + back[:share] + wide(exchange(low(back[share:]), "ctx", 1))
    d_res_one, grad_gain_one, grad_shift_one = normalize_back(d_first, normed_one, inv_one, gain_one)
    d_one_rows = low(d_res_one)
    d_att = low(dot_abt(wout_full, d_one_rows))
    d_parts = [d_att[s * width : (s + 1) * width] for s in range(steps)]
    d_parts = [d_parts[0]] + [rotate(d_parts[s], "tp", -s) for s in range(1, steps)]
    twice = jnp.concatenate(d_parts + d_parts[:-1], 1)
    d_cols = lax.dynamic_slice_in_dim(twice, (steps - t_index) % steps * share, count, 1)

    grad_wdown = dot_atb(activated, d_both)
    grad_win = dot_atb(first_both, d_hidden)
    grad_bin = jnp.sum(wide(d_hidden), 0)
    grad_bout = jnp.sum(wide(d_one_rows), 0)
    grad_wout = dot_ab(attended, d_one_rows)
    grad_vecs = jnp.stack(
        [grad_bout, grad_gain_one, grad_shift_one, grad_bdown, grad_gain_two, grad_shift_two]
    )
    own_win, own_wdown, own_bin, own_wout, own_wproj, own_vecs = reduce_ffn(
        grad_win, grad_wdown, grad_bin, grad_wout, grad_wproj, grad_vecs, core
    )

    d_query, d_kv_y, d_kv_yc = attend_backward(
        seg_own, seg_far, q_cols, d_cols, out_cols, lse, [kv_y, kv_yc], None, False,
        [jnp.float32, jnp.bfloat16],
    )
    d_kv_pair = low(d_kv_y + wide(exchange(d_kv_yc, "ctx", 1)))
    d_kv_far = exchange(d_kv_pair, "ctx", 2)
    d_query, d_kv_own, d_kv_c = attend_backward(
        seg_own, seg_near, q_cols, d_cols, out_cols, lse, [kv_own, kv_c], d_query, True,
        [jnp.float32, jnp.bfloat16],
    )
    d_kv = low(d_kv_own + wide(exchange(d_kv_c, "ctx", 1)) + wide(d_kv_far))

    input_part = low(dot_atbt(d_query, w_q) + dot_abt(d_kv, w_kv))
    piece = lambda j: wide(part(input_part, j % steps, steps, 0))
    total = piece(t_index + steps - 1)
    for s in range(steps - 2, -1, -1):
        total = wide(rotate(low(total), "tp", 1)) + piece(t_index + s)
    input_out = d_res_one + total

    grad_main = jnp.concatenate([dot_atbt(tokens, d_query), dot_atb(tokens, d_kv)], 1)
    grad_bias = jnp.concatenate(
        [jnp.sum(wide(d_query), 1), jnp.zeros((width,), jnp.float32), jnp.sum(wide(d_kv[:, width:]), 0)]
    )
    own_main, sum_bias = reduce_attention(grad_main, grad_bias, core)
    own_wqkv = jnp.stack([own_main[:, i * width : (i + 1) * width] for i in range(3)])
    sums = jnp.stack([sum_bias[:width], sum_bias[2 * width :]]).reshape(2, -1, HD)
    own_battn = part(sums, lax.axis_index("fsdp"), lax.axis_size("fsdp"), 2)

    return (
        embedded[None],
        input_out[None],
        own_wqkv,
        own_battn,
        own_wout,
        own_vecs[0],
        own_vecs[1],
        own_vecs[2],
        own_win,
        own_bin,
        own_wdown,
        own_vecs[3],
        own_vecs[4],
        own_vecs[5],
        own_wproj,
    )


def solution(mesh):
    return jax.shard_map(
        shards,
        mesh=mesh,
        in_specs=(
            P("fsdp", "ctx", None),
            P("fsdp", "ctx"),
            P("fsdp", "ctx", None),
            P(None, "fsdp", "tp"),
            P(None, "tp", "fsdp"),
            P("tp", "fsdp"),
            P("fsdp"),
            P("fsdp"),
            P("fsdp"),
            P("fsdp", "tp"),
            P("tp", "fsdp"),
            P("tp", "fsdp"),
            P("fsdp"),
            P("fsdp"),
            P("fsdp"),
            P("fsdp", None),
        ),
        out_specs=(
            P("fsdp", ("ctx", "tp"), None),
            P("fsdp", ("ctx", "tp"), None),
            P(None, "fsdp", "tp"),
            P(None, "tp", "fsdp"),
            P("tp", "fsdp"),
            P("fsdp"),
            P("fsdp"),
            P("fsdp"),
            P("fsdp", "tp"),
            P("tp", "fsdp"),
            P("tp", "fsdp"),
            P("fsdp"),
            P("fsdp"),
            P("fsdp"),
            P("fsdp", None),
        ),
        check_vma=False,
    )
```

```python
import functools
import jax
import jax.numpy as jnp
from jax import lax
from jax.experimental import pallas as pl
from jax.experimental.pallas import tpu as pltpu
from jax.sharding import PartitionSpec as P


HD = 64
LN_EPS = 1e-05
NORM_EPS = 1e-06
SQRT_HALF = 0.7071067811865476
PDF_SCALE = 0.3989422804014327
SCORE_LOG2 = 0.125 * 1.4426950408889634
MASKED = -1e30
QB = 512
KB = 512
SEGS = 8


def dot_ab(a, b):
    return lax.dot_general(a, b, (((1,), (0,)), ((), ())), preferred_element_type=jnp.float32)


def dot_abt(a, b):
    return lax.dot_general(a, b, (((1,), (1,)), ((), ())), preferred_element_type=jnp.float32)


def eye(rows, cols, shift):
    r = lax.broadcasted_iota(jnp.int32, (rows, cols), 0)
    c = lax.broadcasted_iota(jnp.int32, (rows, cols), 1)
    return jnp.where(r + shift == c, 1.0, 0.0).astype(jnp.bfloat16)


def spread_keys(kv_ref, segk_ref, block, kaug_ref, base, width):
    ident = eye(KB, KB, 0)
    for sub in range(kv_ref.shape[0] // KB):
        rows = pl.ds(sub * KB, KB)
        seg_row = segk_ref[block : block + 1, sub * KB : (sub + 1) * KB]
        tag = lax.broadcasted_iota(jnp.int32, (128, KB), 0) - (width - 128)
        hot = jnp.where(tag == seg_row, 1.0, 0.0).astype(jnp.bfloat16)
        hot_cols = dot_abt(ident, hot).astype(jnp.bfloat16)
        lane = lax.broadcasted_iota(jnp.int32, (KB, 128), 1)
        own = kv_ref[rows, 128:256]
        kaug_ref[pl.ds(base + sub * KB, KB), 0:128] = kv_ref[rows, 0:128]
        kaug_ref[pl.ds(base + sub * KB, KB), 128:256] = jnp.where(
            lane < width - 128, own, hot_cols
        )


def masked_query(q_cols, seg_row, head):
    width = q_cols.shape[0]
    row = lax.broadcasted_iota(jnp.int32, (width, QB), 0)
    inside = (row >= head * HD) & (row < (head + 1) * HD)
    tag = lax.broadcasted_iota(jnp.int32, (256 - width, QB), 0)
    bias = jnp.where((tag < SEGS) & (tag != seg_row), MASKED, 0.0).astype(jnp.bfloat16)
    return jnp.concatenate([jnp.where(inside, q_cols, jnp.zeros_like(q_cols)), bias], 0)


def overlaps(segs_q, q_first, segs_k, block, k_first):
    q_low, q_high = segs_q[0, q_first], segs_q[0, q_first + QB - 1]
    return (segs_k[block, k_first] <= q_high) & (segs_k[block, k_first + KB - 1] >= q_low)


def forward_kernel(nb, steps, first, last, *refs):
    place, segs_q, segs_k, segq_ref, segk_ref, q_ref = refs[:6]
    kv_refs = refs[6 : 6 + nb]
    pos = 6 + nb
    if not first:
        m_in, l_in, acc_in = refs[pos : pos + 3]
        pos += 3
    amount = 2 + steps if last else 3
    outs = refs[pos : pos + amount]
    pos += amount
    kaug_ref, vt_ref, m_ref, l_ref, acc_ref = refs[pos:]
    width = q_ref.shape[0]
    heads = width // HD
    step = pl.program_id(0)
    rows = kv_refs[0].shape[0]
    q_first = step * QB

    @pl.when(step == 0)
    def _():
        pick = eye(width, 2 * width, width)
        for block in range(nb):
            spread_keys(kv_refs[block], segk_ref, block, kaug_ref, block * rows, width)
            for sub in range(rows // KB):
                vt_ref[:, block * rows + sub * KB : block * rows + (sub + 1) * KB] = dot_abt(
                    pick, kv_refs[block][sub * KB : (sub + 1) * KB, :]
                ).astype(jnp.bfloat16)

    if first:
        m_ref[...] = jnp.full_like(m_ref, -3e38)
        l_ref[...] = jnp.zeros_like(l_ref)
        acc_ref[...] = jnp.zeros_like(acc_ref)
    else:
        m_ref[...] = m_in[...]
        l_ref[...] = l_in[...]
        acc_ref[...] = acc_in[...]
    seg_row = segq_ref[0:1, :]
    q_heads = [masked_query(q_ref[...], seg_row, h) for h in range(heads)]
    for block in range(nb):

        def body(sub, carry, block=block):
            @pl.when(overlaps(segs_q, q_first, segs_k, block, sub * KB))
            def _():
                at = pl.multiple_of(block * rows + sub * KB, KB)
                keys = kaug_ref[pl.ds(at, KB), :]
                for h in range(heads):
                    scores = dot_ab(keys, q_heads[h]) * SCORE_LOG2
                    old = m_ref[h : h + 1, :]
                    new = jnp.maximum(old, jnp.max(scores, 0, keepdims=True))
                    probs = jnp.exp2(scores - new)
                    alpha = jnp.exp2(old - new)
                    m_ref[h : h + 1, :] = new
                    l_ref[h : h + 1, :] = l_ref[h : h + 1, :] * alpha + jnp.sum(
                        probs, 0, keepdims=True
                    )
                    acc_ref[h * HD : (h + 1) * HD, :] = acc_ref[
                        h * HD : (h + 1) * HD, :
                    ] * alpha + dot_ab(
                        vt_ref[h * HD : (h + 1) * HD, pl.ds(at, KB)], probs.astype(jnp.bfloat16)
                    )

            return carry

        lax.fori_loop(0, rows // KB, body, 0)
    if last:
        out_ref, lse_ref = outs[:2]
        lse_ref[...] = jnp.zeros_like(lse_ref)
        for h in range(heads):
            total = l_ref[h : h + 1, :]
            out_ref[h * HD : (h + 1) * HD, :] = (
                acc_ref[h * HD : (h + 1) * HD, :] / total
            ).astype(jnp.bfloat16)
            lse_ref[h : h + 1, :] = m_ref[h : h + 1, :] + jnp.log2(total)
        share = outs[2].shape[1]
        for b in range(QB // share):
            relative = lax.rem(step * (QB // share) + b - place[0] + steps, steps)
            for s in range(steps):

                @pl.when(relative == s)
                def _(s=s, b=b):
                    outs[2 + s][...] = out_ref[:, b * share : (b + 1) * share]

    else:
        outs[0][...] = m_ref[...]
        outs[1][...] = l_ref[...]
        outs[2][...] = acc_ref[...]


def attend_forward(place, steps, segs_q, segs_k, q_cols, kvs, carry, last):
    nb = len(kvs)
    width, count = q_cols.shape
    rows = kvs[0].shape[0]
    first = carry is None
    smem = pl.BlockSpec(memory_space=pltpu.SMEM)
    vec = lambda r: pl.BlockSpec((r, QB), lambda i: (0, i))
    whole = lambda a: pl.BlockSpec(a.shape, lambda i: (0, 0))
    args = [place, segs_q, segs_k, segs_q, segs_k, q_cols, *kvs]
    specs = [smem, smem, smem, vec(1), whole(segs_k), vec(width), *[whole(k) for k in kvs]]
    if not first:
        args += list(carry)
        specs += [vec(8), vec(8), vec(width)]
    f32 = jnp.float32
    if last:
        out_shape = (
            jax.ShapeDtypeStruct((width, count), jnp.bfloat16),
            jax.ShapeDtypeStruct((8, count), f32),
            *[jax.ShapeDtypeStruct((width, count // steps), jnp.bfloat16)] * steps,
        )
        out_specs = (
            vec(width),
            vec(8),
            *[pl.BlockSpec((width, count // steps), lambda i: (0, 0))] * steps,
        )
    else:
        out_shape = (
            jax.ShapeDtypeStruct((8, count), f32),
            jax.ShapeDtypeStruct((8, count), f32),
            jax.ShapeDtypeStruct((width, count), f32),
        )
        out_specs = (vec(8), vec(8), vec(width))
    return pl.pallas_call(
        functools.partial(forward_kernel, nb, steps, first, last),
        grid=(count // QB,),
        in_specs=specs,
        out_specs=out_specs,
        out_shape=out_shape,
        scratch_shapes=[
            pltpu.VMEM((nb * rows, 256), jnp.bfloat16),
            pltpu.VMEM((width, nb * rows), jnp.bfloat16),
            pltpu.VMEM((8, QB), f32),
            pltpu.VMEM((8, QB), f32),
            pltpu.VMEM((width, QB), f32),
        ],
        compiler_params=pltpu.CompilerParams(vmem_limit_bytes=24 << 20),
        cost_estimate=pl.CostEstimate(
            flops=count * rows * nb * 6000, bytes_accessed=nb * rows * width * 4,
            transcendentals=0,
        ),
        name="attend_forward",
    )(*args)


def backward_kernel(nb, steps, first, last, *refs):
    place, segs_q, segs_k, segq_ref, segk_ref, q_ref, out_ref, lse_ref = refs[:8]
    d_refs = refs[8 : 8 + steps]
    kv_refs = refs[8 + steps : 8 + steps + nb]
    pos = 8 + steps + nb
    if not first:
        dq_in = refs[pos]
        pos += 1
    dq_ref = refs[pos]
    dkv_refs = refs[pos + 1 : pos + 1 + nb]
    pos += 1 + nb
    kaug_ref, kt_ref, acc_ref, dq_acc, d_all = refs[pos:]
    width = q_ref.shape[0]
    heads = width // HD
    step = pl.program_id(0)
    rows = kv_refs[0].shape[0]
    q_first = step * QB
    bf = jnp.bfloat16

    @pl.when(step == 0)
    def _():
        pick = eye(width, 2 * width, 0)
        acc_ref[...] = jnp.zeros_like(acc_ref)
        share = d_refs[0].shape[1]
        for s in range(steps):
            to = lax.rem(place[0] + s, steps) * share
            d_all[:, pl.ds(pl.multiple_of(to, share), share)] = d_refs[s][...]
        for block in range(nb):
            spread_keys(kv_refs[block], segk_ref, block, kaug_ref, block * rows, width)
            for sub in range(rows // KB):
                kt_ref[:, block * rows + sub * KB : block * rows + (sub + 1) * KB] = dot_abt(
                    pick, kv_refs[block][sub * KB : (sub + 1) * KB, :]
                ).astype(bf)

    seg_row = segq_ref[0:1, :]
    q_cols = q_ref[...]
    d_cols = d_all[:, pl.ds(pl.multiple_of(q_first, QB), QB)]
    ident = eye(QB, QB, 0)
    pad = jnp.zeros((256 - width, QB), bf)
    q_nat = dot_abt(ident, jnp.concatenate([q_cols, pad], 0)).astype(bf)
    d_nat = dot_abt(ident, jnp.concatenate([pad, d_cols], 0)).astype(bf)
    row = lax.broadcasted_iota(jnp.int32, (256, QB), 0)
    lane = lax.broadcasted_iota(jnp.int32, (QB, 256), 1)
    off = 256 - width
    d_full = jnp.concatenate([pad, d_cols], 0)
    zero = jnp.zeros((QB, 256), bf)
    q_heads, q_rows, d_heads, d_rows, deltas = [], [], [], [], []
    for h in range(heads):
        q_heads.append(masked_query(q_cols, seg_row, h))
        q_rows.append(jnp.where((lane >= h * HD) & (lane < (h + 1) * HD), q_nat, zero))
        d_heads.append(
            jnp.where((row >= off + h * HD) & (row < off + (h + 1) * HD), d_full, jnp.zeros_like(d_full))
        )
        d_rows.append(jnp.where((lane >= off + h * HD) & (lane < off + (h + 1) * HD), d_nat, zero))
        part = slice(h * HD, (h + 1) * HD)
        deltas.append(
            jnp.sum(
                d_cols[part, :].astype(jnp.float32) * out_ref[part, :].astype(jnp.float32),
                0,
                keepdims=True,
            )
        )
    if first:
        dq_acc[...] = jnp.zeros_like(dq_acc)
    else:
        dq_acc[...] = dq_in[...]
    for block in range(nb):

        def body(sub, carry, block=block):
            @pl.when(overlaps(segs_q, q_first, segs_k, block, sub * KB))
            def _():
                at = pl.multiple_of(block * rows + sub * KB, KB)
                here = pl.ds(pl.multiple_of(sub * KB, KB), KB)
                keys = kaug_ref[pl.ds(at, KB), :]
                vals = kv_refs[block][here, 2 * width - 256 : 2 * width]
                for h in range(heads):
                    scores = dot_ab(keys, q_heads[h]) * SCORE_LOG2
                    probs = jnp.exp2(scores - lse_ref[h : h + 1, :])
                    d_probs = dot_ab(vals, d_heads[h])
                    d_scores = (probs * (d_probs - deltas[h])).astype(bf)
                    acc_ref[pl.ds(at, KB), 0:256] += dot_ab(d_scores, q_rows[h])
                    acc_ref[pl.ds(at, KB), 2 * width - 256 : 2 * width] += dot_ab(
                        probs.astype(bf), d_rows[h]
                    )
                    part = slice(h * HD, (h + 1) * HD)
                    dq_acc[part, :] += dot_ab(kt_ref[part, pl.ds(at, KB)], d_scores)

            return carry

        lax.fori_loop(0, rows // KB, body, 0)
    if last:
        dq_ref[...] = (dq_acc[...] * 0.125).astype(bf)
    else:
        dq_ref[...] = dq_acc[...]

    @pl.when(step == pl.num_programs(0) - 1)
    def _():
        key_lane = lax.broadcasted_iota(jnp.int32, (KB, 2 * width), 1)
        scale = jnp.where(key_lane < width, 0.125, 1.0)
        for block in range(nb):
            for sub in range(rows // KB):
                dkv_refs[block][sub * KB : (sub + 1) * KB, :] = (
                    acc_ref[block * rows + sub * KB : block * rows + (sub + 1) * KB, :] * scale
                ).astype(dkv_refs[block].dtype)


def attend_backward(place, segs_q, segs_k, q_cols, d_outs, out, lse, kvs, dq, last, types):
    nb = len(kvs)
    width, count = q_cols.shape
    rows = kvs[0].shape[0]
    first = dq is None
    smem = pl.BlockSpec(memory_space=pltpu.SMEM)
    vec = lambda r: pl.BlockSpec((r, QB), lambda i: (0, i))
    whole = lambda a: pl.BlockSpec(a.shape, lambda i: (0, 0))
    steps = len(d_outs)
    args = [place, segs_q, segs_k, segs_q, segs_k, q_cols, out, lse, *d_outs, *kvs]
    specs = [smem, smem, smem, vec(1), whole(segs_k), vec(width), vec(width), vec(8)]
    specs += [whole(k) for k in (*d_outs, *kvs)]
    if not first:
        args.append(dq)
        specs.append(vec(width))
    f32 = jnp.float32
    out_shape = [jax.ShapeDtypeStruct((width, count), jnp.bfloat16 if last else f32)]
    out_shape += [jax.ShapeDtypeStruct((rows, 2 * width), t) for t in types]
    out_specs = [vec(width)] + [whole(k) for k in kvs]
    return pl.pallas_call(
        functools.partial(backward_kernel, nb, steps, first, last),
        grid=(count // QB,),
        in_specs=specs,
        out_specs=out_specs,
        out_shape=out_shape,
        scratch_shapes=[
            pltpu.VMEM((nb * rows, 256), jnp.bfloat16),
            pltpu.VMEM((width, nb * rows), jnp.bfloat16),
            pltpu.VMEM((nb * rows, 2 * width), f32),
            pltpu.VMEM((width, QB), f32),
            pltpu.VMEM((width, count), jnp.bfloat16),
        ],
        compiler_params=pltpu.CompilerParams(vmem_limit_bytes=40 << 20),
        cost_estimate=pl.CostEstimate(
            flops=count * rows * nb * 8000, bytes_accessed=nb * rows * width * 8,
            transcendentals=0,
        ),
        name="attend_backward",
    )(*args)


def tile(rows, cols, at):
    return pl.BlockSpec((rows, cols), lambda i: (at, 0))


def whole_of(a):
    return pl.BlockSpec(a.shape, lambda i: (0,) * len(a.shape))


def run_whole(kernel, args, specs, out_shapes, micros, out_specs=None, aliases=None, scratch=()):
    outs = [jax.ShapeDtypeStruct(s, d) for s, d in out_shapes]
    return pl.pallas_call(
        kernel,
        grid=(1,),
        in_specs=[whole_of(a) if s is None else s for a, s in zip(args, specs)],
        out_specs=out_specs or [whole_of(o) for o in outs],
        out_shape=outs,
        scratch_shapes=list(scratch),
        input_output_aliases=aliases or {},
        compiler_params=pltpu.CompilerParams(vmem_limit_bytes=48 << 20),
        cost_estimate=pl.CostEstimate(
            flops=int(micros * 1e9), bytes_accessed=1 << 20, transcendentals=0
        ),
    )(*args)


def row_mean(value):
    return jnp.mean(value, -1, keepdims=True)


def outer_kernel(steps, *refs):
    head_refs, (x_ref, vec_ref) = refs[:steps], refs[steps : steps + 2]
    own_refs, oth_refs = refs[2 + steps : 2 + 2 * steps], refs[2 + 2 * steps : 2 + 3 * steps]
    low_ref, normed_ref, inv_ref, att_ref = refs[2 + 3 * steps :]
    width, rows = head_refs[0].shape
    ident = eye(rows, rows, 0)
    own = oth = 0.0
    for s in range(steps):
        att_ref[s * width : (s + 1) * width, :] = head_refs[s][...]
        att = low(dot_abt(ident, head_refs[s][...]))
        own += dot_ab(att, own_refs[s][...])
        oth += dot_ab(att, oth_refs[s][...])
    resid = wide(x_ref[...]) + jnp.concatenate([own, oth], 1) + wide(vec_ref[0:1, :])
    centred = resid - row_mean(resid)
    inv = lax.rsqrt(row_mean(centred * centred) + LN_EPS)
    normed = centred * inv
    normed_ref[...] = normed
    inv_ref[...] = jnp.broadcast_to(inv, inv_ref.shape)
    low_ref[...] = low(normed * wide(vec_ref[1:2, :]) + wide(vec_ref[2:3, :]))


def up_kernel(steps, *refs):
    f_ref, g_ref, bias_ref = refs[:3]
    into_own, into_oth, down_own, down_oth = [
        refs[3 + i * steps : 3 + (i + 1) * steps] for i in range(4)
    ]
    mine_ref, send_ref, act_ref, slope_ref = refs[3 + 4 * steps :]
    rows, model = f_ref.shape
    half = model // 2
    unit = into_own[0].shape[1]
    both = jnp.concatenate([f_ref[...], g_ref[...]], 0)
    own = oth = 0.0
    for s in range(steps):
        cut = slice(s * unit, (s + 1) * unit)
        hidden = (
            dot_ab(both[:, :half], into_own[s][...])
            + dot_ab(both[:, half:], into_oth[s][...])
            + bias_ref[0:1, cut]
        )
        cdf = 0.5 * (1.0 + lax.erf(hidden * SQRT_HALF))
        act = low(hidden * cdf)
        act_ref[:, cut] = act
        slope_ref[:, cut] = cdf + hidden * (jnp.exp(-0.5 * hidden * hidden) * PDF_SCALE)
        own += dot_ab(act, down_own[s][...])
        oth += dot_ab(act, down_oth[s][...])
    mine_ref[:, :half] = own[:rows]
    mine_ref[:, half:] = oth[:rows]
    send_ref[:, :half] = low(own[rows:])
    send_ref[:, half:] = low(oth[rows:])


def head_kernel(*refs):
    mine_ref, got_ref, normed_ref, vec_ref, proj_ref, cot_ref = refs[:6]
    embed_ref, d_res_ref, d_low_ref, gproj_ref, gvec_ref = refs[6:]
    first = normed_ref[...] * wide(vec_ref[1:2, :]) + wide(vec_ref[2:3, :])
    resid = first + mine_ref[...] + wide(got_ref[...]) + wide(vec_ref[3:4, :])
    gain = wide(vec_ref[4:5, :])
    centred = resid - row_mean(resid)
    inv = lax.rsqrt(row_mean(centred * centred) + LN_EPS)
    normed = centred * inv
    second = low(normed * gain + wide(vec_ref[5:6, :]))
    weights = proj_ref[...]
    projected = dot_ab(second, weights)
    scale = lax.rsqrt(jnp.sum(projected * projected, -1, keepdims=True) + NORM_EPS)
    embedded = projected * scale
    embed_ref[...] = embedded
    cot = wide(cot_ref[...])
    d_proj = low(scale * (cot - embedded * jnp.sum(embedded * cot, -1, keepdims=True)))
    ident = eye(d_proj.shape[1], d_proj.shape[1], 0)
    gproj_ref[...] = dot_ab(low(dot_abt(ident, d_proj)), second)
    d_second = dot_abt(d_proj, weights)
    scaled = d_second * gain
    d_res = inv * (scaled - row_mean(scaled) - normed * row_mean(scaled * normed))
    d_res_ref[...] = d_res
    d_low = low(d_res)
    d_low_ref[...] = d_low
    gvec_ref[...] = jnp.zeros_like(gvec_ref)
    gvec_ref[3:4, :] = jnp.sum(wide(d_low), 0, keepdims=True)
    gvec_ref[4:5, :] = jnp.sum(d_second * normed, 0, keepdims=True)
    gvec_ref[5:6, :] = jnp.sum(d_second, 0, keepdims=True)


def down_kernel(steps, *refs):
    f_ref, g_ref, d_ref, e_ref, act_ref, slope_ref = refs[:6]
    into_own, into_oth, down_own, down_oth = [
        refs[6 + i * steps : 6 + (i + 1) * steps] for i in range(4)
    ]
    pos = 6 + 4 * steps
    mine_ref, send_ref, bias_ref = refs[pos : pos + 3]
    own_refs, oth_refs = refs[pos + 3 : pos + 3 + steps], refs[pos + 3 + steps :]
    rows, model = f_ref.shape
    half = model // 2
    unit = into_own[0].shape[1]
    d_both = jnp.concatenate([d_ref[...], e_ref[...]], 0)
    both = jnp.concatenate([f_ref[...], g_ref[...]], 0)
    bias_ref[...] = jnp.zeros_like(bias_ref)
    own = oth = 0.0
    for s in range(steps):
        cut = slice(s * unit, (s + 1) * unit)
        d_act = dot_abt(d_both[:, :half], down_own[s][...]) + dot_abt(
            d_both[:, half:], down_oth[s][...]
        )
        d_hidden = low(d_act * slope_ref[:, cut])
        bias_ref[0:1, cut] = jnp.sum(wide(d_hidden), 0, keepdims=True)
        own += dot_abt(d_hidden, into_own[s][...])
        oth += dot_abt(d_hidden, into_oth[s][...])
        into = low(dot_atb(both, d_hidden))
        own_refs[s][0:half, :] = into[:half]
        oth_refs[s][0:half, :] = into[half:]
        down = low(dot_atb(act_ref[:, cut], d_both))
        own_refs[s][half : half + unit, :] = down[:, :half]
        oth_refs[s][half : half + unit, :] = down[:, half:]
    mine_ref[:, :half] = own[:rows]
    mine_ref[:, half:] = oth[:rows]
    send_ref[:, :half] = low(own[rows:])
    send_ref[:, half:] = low(oth[rows:])


def inner_kernel(steps, *refs):
    d_res_ref, mine_ref, got_ref, normed_ref, inv_ref, vec_ref, gproj_ref, gvec_ref = refs[:8]
    own_refs, oth_refs = refs[8 : 8 + steps], refs[8 + steps : 8 + 2 * steps]
    d_one_ref, pack_ref = refs[8 + 2 * steps : 10 + 2 * steps]
    att_refs = refs[10 + 2 * steps :]
    rows, model = d_res_ref.shape
    half = model // 2
    normed = normed_ref[...]
    d_first = d_res_ref[...] + mine_ref[...] + wide(got_ref[...])
    scaled = d_first * wide(vec_ref[1:2, :])
    d_one = inv_ref[:, 0:1] * (scaled - row_mean(scaled) - normed * row_mean(scaled * normed))
    d_one_ref[...] = d_one
    d_low = low(d_one)
    pack_ref[0:rows, :] = d_low
    embed = gproj_ref.shape[0]
    pack_ref[rows : rows + embed, :] = low(gproj_ref[...])
    sums = [
        jnp.sum(wide(d_low), 0, keepdims=True),
        jnp.sum(d_first * normed, 0, keepdims=True),
        jnp.sum(d_first, 0, keepdims=True),
    ]
    vecs = jnp.concatenate([*sums, gvec_ref[3:6, :], jnp.zeros((10, model), jnp.float32)], 0)
    pack_ref[rows + embed : rows + embed + 16, :] = low(vecs)
    for s in range(steps):
        att_refs[s][...] = low(
            dot_abt(own_refs[s][...], d_low[:, :half]) + dot_abt(oth_refs[s][...], d_low[:, half:])
        )


def outer_grad_kernel(steps, *refs):
    place, mine_ref, got_ref, att_ref, natt_ref, bias_ref = refs[:6]
    outs = refs[6 + 2 * steps :]
    own_refs, oth_refs = outs[:steps], outs[steps:]
    rows = att_ref.shape[1]
    model = mine_ref.shape[1]
    half = model // 2
    embed = mine_ref.shape[0] - rows - 16
    width = att_ref.shape[0] // steps
    core = place[1]
    d_mine, d_got = mine_ref[0:rows, :], got_ref[0:rows, :]
    at = pl.multiple_of(rows + core * (embed // 2), 16)
    proj = low(
        wide(mine_ref[pl.ds(at, embed // 2), :]) + wide(got_ref[pl.ds(at, embed // 2), :])
    )
    vecs = wide(mine_ref[rows + embed :, :]) + wide(got_ref[rows + embed :, :])
    line = lax.broadcasted_iota(jnp.int32, (16, half), 0)
    unit = bias_ref.shape[1] // steps
    for s in range(steps):
        cut = pl.ds(pl.multiple_of(s * width + core * (width // 2), 16), width // 2)
        grad = low(dot_ab(att_ref[cut, :], d_mine) + dot_ab(natt_ref[cut, :], d_got))
        bias = bias_ref[0:1, s * unit : (s + 1) * unit]
        for refs_of, lanes in ((own_refs, slice(0, half)), (oth_refs, slice(half, model))):
            out = refs_of[s]
            a, b = width // 2, width // 2 + embed // 2
            out[0:a, :] = grad[:, lanes]
            out[a:b, :] = proj[:, lanes]
            out[b : b + 16, :] = low(jnp.where(line == 6, bias, vecs[:, lanes]))
            out[b + 16 :, :] = jnp.zeros((out.shape[0] - b - 16, half), jnp.bfloat16)


def exchange(value, axis, flip):
    size = lax.axis_size(axis)
    return lax.ppermute(value, axis, [(i, i ^ flip) for i in range(size)])


def rotate(value, axis, amount):
    size = lax.axis_size(axis)
    return lax.ppermute(value, axis, [(i, (i + amount) % size) for i in range(size)])


def in_order(index, own, other, dim):
    first = index == 0
    return jnp.concatenate([jnp.where(first, own, other), jnp.where(first, other, own)], dim)


def part(array, index, count, dim):
    size = array.shape[dim] // count
    return lax.dynamic_slice_in_dim(array, index * size, size, dim)


def pad_to(array, rows, cols):
    return jnp.pad(array, ((0, rows - array.shape[0]), (0, cols - array.shape[1])))


def low(value):
    return value.astype(jnp.bfloat16)


def wide(value):
    return value.astype(jnp.float32)


def after(value, other):
    return lax.optimization_barrier((value, other))[0]


def sum_pair(value, axis, flip):
    rounded = low(value)
    return wide(rounded) + wide(exchange(rounded, axis, flip))


def dot_atb(a, b):
    return lax.dot_general(a, b, (((0,), (0,)), ((), ())), preferred_element_type=jnp.float32)


def dot_atbt(a, b):
    return lax.dot_general(a, b, (((0,), (1,)), ((), ())), preferred_element_type=jnp.float32)


def paired():
    return lax.axis_size("fsdp") == 2


def side_of():
    return lax.axis_index("fsdp") if paired() else 0


def turn(array):
    if not paired():
        return array
    half = array.shape[-1] // 2
    first = side_of() == 0
    lower, upper = array[..., :half], array[..., half:]
    return jnp.concatenate([jnp.where(first, lower, upper), jnp.where(first, upper, lower)], -1)


def gather_attention(w_qkv, b_attn, w_proj, vectors, core):
    width = w_qkv.shape[2]
    main = jnp.concatenate([w_qkv[0], w_qkv[1], w_qkv[2], w_proj], 1)
    cols = main.shape[1]
    bias = b_attn.reshape(2 * b_attn.shape[1], b_attn.shape[2])
    if not paired():
        weights = lax.all_gather(main, "fsdp", axis=0, tiled=True)
        vecs = lax.all_gather(vectors, "fsdp", axis=1, tiled=True)
        biases = lax.all_gather(bias, "fsdp", axis=1, tiled=True)
        return weights, vecs, biases.reshape(2, width), weights
    half = main.shape[0] // 2
    wide_cols = -(-cols // 128) * 128
    small = jnp.concatenate([pad_to(vectors, 8, wide_cols), pad_to(bias, 8, wide_cols)], 0)
    packed = jnp.concatenate([pad_to(part(main, core, 2, 0), half, wide_cols), small], 0)
    got = exchange(packed, "fsdp", 1)
    got_half = got[:half]
    partner_half = exchange(got_half, "ctx", 1)
    other = in_order(core, got_half, partner_half, 0)[:, :cols]
    weights = jnp.concatenate([main, other], 0)
    length = vectors.shape[1]
    vecs = jnp.concatenate([vectors, got[half : half + 8, :length]], 1)
    got_bias = got[half + 8 : half + 8 + bias.shape[0], : bias.shape[1]]
    biases = in_order(side_of(), bias, got_bias, 1)
    return weights, vecs, biases.reshape(2, width), got


def gather_ffn(w_in, w_down, w_out, b_in, core, gate):
    steps = lax.axis_size("tp")
    rows, _ = b_in.shape
    into = part(w_in, core, 2, 1)
    down = part(w_down, core, 2, 0)
    if not paired():
        into = lax.all_gather(into, "fsdp", axis=0, tiled=True)
        down = lax.all_gather(down, "fsdp", axis=1, tiled=True)
        outer = lax.all_gather(w_out, "fsdp", axis=1, tiled=True)
        bias = lax.all_gather(b_in, "fsdp", axis=1, tiled=True)
        half = into.shape[0] // 2
        halves = []
        for i in range(2):
            cut = slice(i * half, (i + 1) * half)
            bias_half = bias[:, i * HD // 2 : (i + 1) * HD // 2].reshape(1, -1)
            halves.append(
                jnp.concatenate(
                    [into[cut], down[:, cut], outer[:, cut], pad_to(bias_half, 16, half)], 0
                )
            )
        owns, others = [halves[0]], [halves[1]]
        for _ in range(steps - 1):
            owns.append(rotate(owns[-1], "tp", 1))
            others.append(rotate(others[-1], "tp", 1))
    else:
        depth = w_in.shape[0]
        bias_row = pad_to(b_in.reshape(1, -1), 16, depth)
        owns = [jnp.concatenate([into, down, w_out, bias_row], 0)]
        for _ in range(1, steps):
            owns.append(rotate(owns[-1], "tp", 1))
        others = []
        for s in range(steps):
            others.append(exchange(after(owns[s], gate), "fsdp", 1))
    at = owns[0].shape[0] - 16
    line = lambda packs: jnp.concatenate([p[at : at + 1] for p in packs], 0).reshape(
        steps, rows, HD // 2
    )
    bias = in_order(side_of(), line(owns), line(others), 2)
    return owns, others, wide(part(bias, core, 2, 1)).reshape(1, -1)


def reduce_ffn(owns, others, core, width, embed):
    steps = len(owns)
    depth = owns[0].shape[1]
    unit = depth
    total = None
    if paired():
        row = lax.axis_index("ctx") // 2
        for s in range(steps - 1, -1, -1):
            got = exchange(others[s], "fsdp", 1)
            halved = lambda a, i: wide(part(a, i, 2, 0))
            sent = low(halved(owns[s], 1 - row) + halved(got, 1 - row))
            here = halved(owns[s], row) + halved(got, row)
            here = here + wide(exchange(sent, "ctx", 2))
            if total is not None:
                here = here + wide(rotate(total, "tp", -1))
            total = low(here)
        total = in_order(row, total, exchange(total, "ctx", 2), 0)
        partner = exchange(total, "ctx", 1)
        both = lambda a, b, d: wide(in_order(core, total[a:b], partner[a:b], d))
        into, down = both(0, depth, 1), both(depth, depth + unit, 0)
        small = total[depth + unit :]
        small_partner = partner[depth + unit :]
    else:
        scatter = lambda a, d: lax.psum_scatter(a, "fsdp", scatter_dimension=d, tiled=True)
        add = lambda a, b: low(wide(a) + wide(b))
        for s in range(steps - 1, -1, -1):
            cut = slice(depth, depth + unit)
            rest = [p[depth + unit :] for p in (owns[s], others[s])]
            line = rest[0][width // 2 + embed // 2 + 6 :][:1]
            parts = (
                scatter(jnp.concatenate([owns[s][:depth], others[s][:depth]], 0), 0),
                scatter(jnp.concatenate([owns[s][cut], others[s][cut]], 1), 1),
                scatter(jnp.concatenate(rest, 1), 1),
                lax.psum(line, "fsdp"),
            )
            if total is not None:
                parts = tuple(add(a, rotate(b, "tp", -1)) for a, b in zip(parts, total))
            total = parts
        total = [low(sum_pair(a, "ctx", 2)) for a in total]
        partner = [exchange(a, "ctx", 1) for a in total]
        into = wide(in_order(core, total[0], partner[0], 1))
        down = wide(in_order(core, total[1], partner[1], 0))
        small, small_partner = total[2], partner[2]
    a = width // 2
    b = a + embed // 2
    outer = wide(in_order(core, small[:a], small_partner[:a], 0))
    proj = wide(in_order(core, small[a:b], small_partner[a:b], 0)).T
    vecs = wide(small[b : b + 6])
    if paired():
        lines = in_order(core, small[b + 6 : b + 7], small_partner[b + 6 : b + 7], 0)
    else:
        lines = in_order(core, total[3], partner[3], 0)
    bias = part(
        wide(lines).reshape(-1, HD), lax.axis_index("fsdp"), lax.axis_size("fsdp"), 1
    )
    return into, down, bias, outer, proj, vecs


def reduce_attention(g_main, g_bias, core):
    model, cols = g_main.shape
    bias = pad_to(g_bias.reshape(1, -1), 16, cols)
    if not paired():
        own = lax.psum_scatter(low(g_main), "fsdp", scatter_dimension=0, tiled=True)
        shared = lax.psum(low(bias), "fsdp")
        both = jnp.concatenate([own, shared], 0)
        both = low(sum_pair(both, "ctx", 1))
        both = sum_pair(both, "ctx", 2)
        count = own.shape[0]
        return wide(low(both[:count])), both[count]
    quarter = model // 4
    quads = low(g_main).reshape(2, 2, quarter, cols)
    take = lambda a, i, d: lax.dynamic_index_in_dim(a, i, d, keepdims=False)
    mine, sent = take(quads, core, 1), take(quads, 1 - core, 1)
    got = exchange(
        jnp.concatenate([sent.reshape(2 * quarter, cols), low(bias)], 0), "ctx", 1
    )
    halves = wide(mine) + wide(got[: 2 * quarter]).reshape(2, quarter, cols)
    bias = low(wide(low(bias)) + wide(got[2 * quarter :]))
    got = exchange(jnp.concatenate([low(halves[1]), bias], 0), "fsdp", 1)
    own = halves[0] + wide(got[:quarter])
    bias = low(wide(bias) + wide(got[quarter:]))
    both = low(sum_pair(jnp.concatenate([low(own), bias], 0), "ctx", 2))
    other = exchange(both[:quarter], "ctx", 1)
    return wide(in_order(core, both[:quarter], other, 0)), wide(both[quarter])


def layer(
    layer_input,
    segments,
    cotangent,
    w_qkv,
    b_attn,
    w_out,
    b_out,
    ln1_gain,
    ln1_bias,
    w_in,
    b_in,
    w_down,
    b_down,
    ln2_gain,
    ln2_bias,
    w_proj,
):
    _, count, model = layer_input.shape
    width = w_qkv.shape[2]
    embed = w_proj.shape[1]
    half = model // 2
    steps = lax.axis_size("tp")
    share = count // steps
    t_index = lax.axis_index("tp")
    core = lax.axis_index("ctx") % 2
    place = jnp.stack([t_index, core])
    bf, f32 = jnp.bfloat16, jnp.float32
    tokens = turn(layer_input.reshape(count, model))
    own_tokens = part(tokens, t_index, steps, 0)
    upstream = part(cotangent.reshape(count, -1), t_index, steps, 0)

    seg_own = segments.reshape(1, count)
    vectors = jnp.stack(
        [b_out, ln1_gain, ln1_bias, b_down, ln2_gain, ln2_bias, b_out, b_out]
    )
    weights, vecs, biases, gate = gather_attention(w_qkv, b_attn, w_proj, vectors, core)
    seg_y = exchange(seg_own, "ctx", 2)
    seg_pair = exchange(jnp.concatenate([seg_own, seg_y], 0), "ctx", 1)
    seg_near = jnp.concatenate([seg_own, seg_pair[0:1]], 0)
    seg_far = jnp.concatenate([seg_y, seg_pair[1:2]], 0)

    w_q, w_kv = weights[:, :width], weights[:, width : 3 * width]
    wproj_full = weights[:, 3 * width :]
    kv_bias = jnp.concatenate([jnp.zeros((width,), f32), wide(biases[1])])
    kv_own = low(dot_ab(tokens, w_kv) + kv_bias)
    kv_y = exchange(kv_own, "ctx", 2)
    kv_c = exchange(kv_own, "ctx", 1)
    q_cols = low(dot_atbt(w_q, tokens) + wide(biases[0])[:, None])
    kv_yc = exchange(kv_y, "ctx", 1)
    owns, others, bin_row = gather_ffn(w_in, w_down, w_out, b_in, core, gate)

    carry = attend_forward(place, steps, seg_own, seg_near, q_cols, [kv_own, kv_c], None, False)
    out_cols, lse, *cuts = attend_forward(
        place, steps, seg_own, seg_far, q_cols, [kv_y, kv_yc], carry, True
    )
    heads = [cuts[0]] + [rotate(cuts[s], "tp", s) for s in range(1, steps)]

    unit = half
    outer_specs = [tile(width, half, 2 * half // width)] * (2 * steps)
    ffn_specs = [tile(half, half, 0)] * (2 * steps) + [tile(half, half, 1)] * (2 * steps)
    first_low, normed_one, inv_one, attended = run_whole(
        functools.partial(outer_kernel, steps),
        [*heads, own_tokens, vecs, *owns, *others], [None] * (2 + steps) + outer_specs,
        [
            ((share, model), bf),
            ((share, model), f32),
            ((share, 128), f32),
            ((steps * width, share), bf),
        ],
        4,
    )
    first_near = exchange(first_low, "ctx", 1)
    part_mine, part_send, activated, slope = run_whole(
        functools.partial(up_kernel, steps),
        [first_low, first_near, bin_row, *owns, *others, *owns, *others],
        [None] * 3 + ffn_specs,
        [
            ((share, model), f32),
            ((share, model), bf),
            ((2 * share, steps * unit), bf),
            ((2 * share, steps * unit), f32),
        ],
        8,
    )
    embedded, d_res_two, d_rows, grad_proj, grad_vecs = run_whole(
        head_kernel,
        [part_mine, exchange(part_send, "ctx", 1), normed_one, vecs, wproj_full, upstream],
        [None] * 6,
        [
            ((share, embed), f32),
            ((share, model), f32),
            ((share, model), bf),
            ((embed, model), f32),
            ((8, model), f32),
        ],
        4,
    )
    d_near = exchange(d_rows, "ctx", 1)
    pack_rows = 2 * half + width
    back_mine, back_send, grad_bin, *packs = run_whole(
        functools.partial(down_kernel, steps),
        [first_low, first_near, d_rows, d_near, activated, slope,
         *owns, *others, *owns, *others],
        [None] * 6 + ffn_specs,
        [((share, model), f32), ((share, model), bf), ((8, steps * unit), f32)]
        + [((pack_rows, half), bf)] * (2 * steps),
        12,
    )
    d_res_one, pair_rows, *d_cuts = run_whole(
        functools.partial(inner_kernel, steps),
        [d_res_two, back_mine, exchange(back_send, "ctx", 1), normed_one, inv_one, vecs,
         grad_proj, grad_vecs, *owns, *others],
        [None] * 8 + outer_specs,
        [((share, model), f32), ((share + embed + 16, model), bf)]
        + [((width, share), bf)] * steps,
        4,
    )
    d_cuts = [d_cuts[0]] + [rotate(d_cuts[s], "tp", -s) for s in range(1, steps)]
    packs = run_whole(
        functools.partial(outer_grad_kernel, steps),
        [place, pair_rows, exchange(pair_rows, "ctx", 1), attended,
         exchange(attended, "ctx", 1), grad_bin, *packs],
        [pl.BlockSpec(memory_space=pltpu.SMEM)] + [None] * 5
        + [pl.BlockSpec(memory_space=pl.ANY)] * (2 * steps),
        [((pack_rows, half), bf)] * (2 * steps), 3,
        out_specs=[tile(width, half, 2 * half // width)] * (2 * steps),
        aliases={6 + i: i for i in range(2 * steps)},
    )
    own_win, own_wdown, own_bin, own_wout, own_wproj, own_vecs = reduce_ffn(
        packs[:steps], packs[steps:], core, width, embed
    )

    d_query, d_kv_y, d_kv_yc = attend_backward(
        place, seg_own, seg_far, q_cols, d_cuts, out_cols, after(lse, packs[0]),
        [kv_y, kv_yc], None, False, [f32, bf],
    )
    d_kv_pair = low(d_kv_y + wide(exchange(d_kv_yc, "ctx", 1)))
    d_kv_far = exchange(d_kv_pair, "ctx", 2)
    d_query, d_kv_own, d_kv_c = attend_backward(
        place, seg_own, seg_near, q_cols, d_cuts, out_cols, lse, [kv_own, kv_c], d_query,
        True, [f32, bf],
    )
    d_kv = low(d_kv_own + wide(exchange(d_kv_c, "ctx", 1)) + wide(d_kv_far))

    input_part = low(dot_atbt(d_query, w_q) + dot_abt(d_kv, w_kv))
    piece = lambda j: wide(part(input_part, j % steps, steps, 0))
    total = piece(t_index + steps - 1)
    for s in range(steps - 2, -1, -1):
        total = wide(rotate(low(total), "tp", 1)) + piece(t_index + s)
    input_out = turn(d_res_one + total)

    grad_main = jnp.concatenate([dot_atbt(tokens, d_query), dot_atb(tokens, d_kv)], 1)
    grad_bias = jnp.concatenate(
        [jnp.sum(wide(d_query), 1), jnp.zeros((width,), f32), jnp.sum(wide(d_kv[:, width:]), 0)]
    )
    own_main, sum_bias = reduce_attention(grad_main, grad_bias, core)
    own_wqkv = jnp.stack([own_main[:, i * width : (i + 1) * width] for i in range(3)])
    sums = jnp.stack([sum_bias[:width], sum_bias[2 * width :]]).reshape(2, -1, HD)
    own_battn = part(sums, lax.axis_index("fsdp"), lax.axis_size("fsdp"), 2)

    return (
        embedded[None],
        input_out[None],
        own_wqkv,
        own_battn,
        own_wout,
        own_vecs[0],
        own_vecs[1],
        own_vecs[2],
        own_win,
        own_bin,
        own_wdown,
        own_vecs[3],
        own_vecs[4],
        own_vecs[5],
        own_wproj,
    )


def solution(mesh):
    return jax.shard_map(
        layer,
        mesh=mesh,
        in_specs=(
            P("fsdp", "ctx", None),
            P("fsdp", "ctx"),
            P("fsdp", "ctx", None),
            P(None, "fsdp", "tp"),
            P(None, "tp", "fsdp"),
            P("tp", "fsdp"),
            P("fsdp"),
            P("fsdp"),
            P("fsdp"),
            P("fsdp", "tp"),
            P("tp", "fsdp"),
            P("tp", "fsdp"),
            P("fsdp"),
            P("fsdp"),
            P("fsdp"),
            P("fsdp", None),
        ),
        out_specs=(
            P("fsdp", ("ctx", "tp"), None),
            P("fsdp", ("ctx", "tp"), None),
            P(None, "fsdp", "tp"),
            P(None, "tp", "fsdp"),
            P("tp", "fsdp"),
            P("fsdp"),
            P("fsdp"),
            P("fsdp"),
            P("fsdp", "tp"),
            P("tp", "fsdp"),
            P("tp", "fsdp"),
            P("fsdp"),
            P("fsdp"),
            P("fsdp"),
            P("fsdp", None),
        ),
        check_vma=False,
    )
```
